128 devices in a mesh: rows: 4 (over x), cols: 8 (over z, core), slabs: 4 (over y).
Axes of the slice: x: 4, y: 4, z: 4, core: 2. Of those that a mesh axis runs over, the one named last changes fastest.
Arguments:
- field_values: float32 [16, 256, 512, 128], P('rows', 'cols', 'slabs'), may hold values from 0.5 to 2
- mobility: float32 [16, 256, 512, 128], P('rows', 'cols', 'slabs'), may hold values from 0.03 to 0.15
- source: float32 [16, 256, 512, 128], P('rows', 'cols', 'slabs'), may hold values from -0.2 to 0.2
Outputs:
- anomaly: float32 [16, 256, 512, 128], P('rows', 'cols', 'slabs')
- field_values_end: float32 [16, 256, 512, 128], P('rows', 'cols', 'slabs')
The draws below stay inside these ranges and needn't reach their ends.
All inputs are finite; a program needn't handle non-finite values.
Results may differ from the reference program's by a relative error of at most 0.00002.
Values sent between devices are 32-bit elements; how exact they have to be, the bound alone decides.
A program may use at most 128 MiB of HBM per device.

```python
import jax
import jax.numpy as jnp
from jax import lax

GRID_Y = 16
GRID_X = 256
GRID_Z = 512
LEVELS = 128
STEPS = 3


def shard_levels(stream_key, shape, split, least, largest):
    factor_of = 1.0
    for axis_at, shards_of in split:
        steps = jax.random.uniform(jax.random.fold_in(jax.random.fold_in(stream_key, 6), axis_at), (shards_of,), jnp.float32, least / len(split), largest / len(split))
        factor_of = factor_of * jnp.repeat(jnp.exp(steps), shape[axis_at] // shards_of).reshape((-1,) + (1,) * (len(shape) - 1 - axis_at))
    return factor_of


def setup_inputs(seed: int = 0) -> dict:
    splits = jax.random.split(jax.random.key(seed), 4)
    return {
        "field_values": jnp.clip(0.5 + 1.5 * jax.random.uniform(splits[0], (GRID_Y, GRID_X, GRID_Z, LEVELS), jnp.float32) ** shard_levels(splits[0], (GRID_Y, GRID_X, GRID_Z, LEVELS), ((0, 4), (1, 8), (2, 4)), -0.2, 0.2), 0.5, 2.0),
        "mobility": jnp.clip(0.03 + 0.120000007 * jax.random.uniform(splits[1], (GRID_Y, GRID_X, GRID_Z, LEVELS), jnp.float32) ** shard_levels(splits[1], (GRID_Y, GRID_X, GRID_Z, LEVELS), ((0, 4), (1, 8), (2, 4)), -0.2, 0.2), 0.03, 0.15),
        "source": jnp.clip(jax.random.uniform(splits[2], (GRID_Y, GRID_X, GRID_Z, LEVELS), jnp.float32, -0.2, 0.2) * shard_levels(splits[2], (GRID_Y, GRID_X, GRID_Z, LEVELS), ((0, 4), (1, 8), (2, 4)), -0.4, 0.0), -0.2, 0.2),
    }


def strip_edges(values, dims):
    for dim in dims:
        values = lax.slice_in_dim(values, 1, values.shape[dim] - 1, axis=dim)
    return values

def neighbour(values, dim, start, dims):
    others = [other for other in dims if other != dim]
    values = strip_edges(values, others)
    return lax.slice_in_dim(values, start, start + values.shape[dim] - 2, axis=dim)

def one_step(padded, mobility, source):
    middle = strip_edges(padded, (0, 1, 2))
    lower = [neighbour(padded, dim, 0, (0, 1, 2)) for dim in (0, 1, 2)]
    upper = [neighbour(padded, dim, 2, (0, 1, 2)) for dim in (0, 1, 2)]
    spread = lower[0] + upper[0] + lower[1] + upper[1] + lower[2] + upper[2] - 6.0 * middle
    return middle + mobility * spread + source

def reference(field_values, mobility, source):
    for step in range(STEPS):
        field_values = one_step(jnp.pad(field_values, ((1, 1), (1, 1), (1, 1), (0, 0)), mode='wrap'), mobility, source)
    line_mean = lax.optimization_barrier(jnp.mean(field_values, axis=2, keepdims=True))
    centred = field_values - line_mean
    line_variance = lax.optimization_barrier(jnp.mean(centred * centred, axis=2, keepdims=True))
    anomaly = centred * lax.rsqrt(line_variance + 0.0001)
    return (anomaly, field_values)
```

```python
import functools

import jax
import jax.numpy as jnp
from jax import lax
from jax.experimental import pallas as pl
from jax.experimental.pallas import tpu as pltpu
from jax.sharding import PartitionSpec as P

STEPS = 3
LINES = 2
EPS = 1e-4
MESH = pl.DeviceIdType.MESH
DMA = pltpu.SemaphoreType.DMA


def ring(axis, by):
    size = lax.axis_size(axis)
    return {axis: lax.rem(lax.axis_index(axis) + by % size, size)}


def remote(src, dst, send, recv, to):
    return pltpu.make_async_remote_copy(
        src_ref=src, dst_ref=dst, send_sem=send, recv_sem=recv, device_id=to, device_id_type=MESH
    )


def steps_kernel(
    field, mobility, source, odd, stats,
    even, mob, src, z_low, z_high, z_out,
    y_send, y_recv, x_send, x_recv, z_send, z_recv, s_send, s_recv, local,
):
    ny, nx, nz, _ = field.shape
    pieces = nx // LINES
    slabs = lax.axis_size("slabs")
    peers = [ring("rows", 1), ring("rows", -1), ring("cols", 1), ring("cols", -1)]
    peers += [ring("slabs", d) for d in range(1, slabs)]

    loads = [
        pltpu.make_async_copy(field, even.at[pl.ds(1, ny), pl.ds(1, nx)], local.at[0]),
        pltpu.make_async_copy(mobility, mob, local.at[1]),
        pltpu.make_async_copy(source, src, local.at[2]),
    ]
    barrier = pltpu.get_barrier_semaphore()
    for peer in peers:
        pl.semaphore_signal(barrier, inc=1, device_id=peer, device_id_type=MESH)
    for load in loads:
        load.start()
    pl.semaphore_wait(barrier, len(peers))

    def y_copies(n, c):
        buf = odd if n % 2 else even
        lines = pl.ds(1 + c * LINES, LINES)
        if n:
            first, last = buf.at[1, lines], buf.at[ny, lines]
        else:
            first, last = field.at[0, pl.ds(c * LINES, LINES)], field.at[ny - 1, pl.ds(c * LINES, LINES)]
        return (
            remote(last, buf.at[0, lines], y_send.at[n, 0, c], y_recv.at[n, 0, c], ring("rows", 1)),
            remote(first, buf.at[ny + 1, lines], y_send.at[n, 1, c], y_recv.at[n, 1, c], ring("rows", -1)),
        )

    def x_copies(n):
        buf = odd if n % 2 else even
        planes = pl.ds(1, ny)
        if n:
            first, last = buf.at[planes, 1], buf.at[planes, nx]
        else:
            first, last = field.at[:, 0], field.at[:, nx - 1]
        return (
            remote(last, buf.at[planes, 0], x_send.at[n, 0], x_recv.at[n, 0], ring("cols", 1)),
            remote(first, buf.at[planes, nx + 1], x_send.at[n, 1], x_recv.at[n, 1], ring("cols", -1)),
        )

    def z_copies(n):
        return (
            remote(z_out.at[n, 0], z_low.at[n], z_send.at[n, 0], z_recv.at[n, 0], ring("slabs", 1)),
            remote(z_out.at[n, 1], z_high.at[n], z_send.at[n, 1], z_recv.at[n, 1], ring("slabs", -1)),
        )

    def stat_copies(c):
        return [
            remote(stats.at[0, c], stats.at[d, c], s_send.at[d - 1, c], s_recv.at[d - 1, c], ring("slabs", d))
            for d in range(1, slabs)
        ]

    def start(copies):
        for copy in copies:
            copy.start()

    def arrived(copies):
        for copy in copies:
            copy.wait_recv()

    def sent(copies):
        for copy in copies:
            copy.wait_send()

    def each(count, body):
        def step(i, carry):
            body(i)
            return carry

        lax.fori_loop(0, count, step, 0)

    start(x_copies(0))
    each(pieces, lambda c: start(y_copies(0, c)))
    loads[0].wait()

    def pack(i):
        for y in range(ny):
            z_out[0, 0, y, pl.ds(i, 1)] = even[y + 1, i + 1, pl.ds(nz - 1, 1)]
            z_out[0, 1, y, pl.ds(i, 1)] = even[y + 1, i + 1, pl.ds(0, 1)]

    each(nx, pack)
    start(z_copies(0))
    loads[1].wait()
    loads[2].wait()

    row = lax.broadcasted_iota(jnp.int32, (nz, 128), 0)

    def one_line(n, y, i):
        old, new = (odd, even) if n % 2 else (even, odd)
        middle = old[y + 1, i + 1]
        low = jnp.where(row == 0, z_low[n, y, pl.ds(i, 1)], pltpu.roll(middle, 1, 0))
        high = jnp.where(row == nz - 1, z_high[n, y, pl.ds(i, 1)], pltpu.roll(middle, nz - 1, 0))
        spread = old[y, i + 1] + old[y + 2, i + 1] + old[y + 1, i] + old[y + 1, i + 2] + low + high - 6.0 * middle
        value = middle + mob[y, i] * spread + src[y, i]
        new[y + 1, i + 1] = value
        if n + 1 < STEPS:
            z_out[n + 1, 0, y, pl.ds(i, 1)] = value[nz - 1:]
            z_out[n + 1, 1, y, pl.ds(i, 1)] = value[:1]
        return value

    def line_stats(value, c, k, y):
        mean = jnp.sum(value, axis=0, keepdims=True) * (1.0 / nz)
        centred = value - mean
        at = pl.ds(k * ny + y, 1)
        stats[0, c, 0, at] = mean
        stats[0, c, 1, at] = jnp.sum(centred * centred, axis=0, keepdims=True)

    for n in range(STEPS - 1):
        arrived(x_copies(n))
        arrived(z_copies(n))

        def inner(i):
            for y in range(1, ny - 1):
                one_line(n, y, i)

        def outer(c):
            arrived(y_copies(n, c))
            for k in range(LINES):
                for y in (0, ny - 1):
                    one_line(n, y, c * LINES + k)

        def outer_and_send(c):
            outer(c)
            start(y_copies(n + 1, c - 1))

        each(nx, inner)
        outer(0)
        lax.fori_loop(1, pieces, lambda c, carry: (outer_and_send(c), carry)[1], 0)
        start(x_copies(n + 1))
        start(z_copies(n + 1))
        start(y_copies(n + 1, pieces - 1))

    n = STEPS - 1
    sent(x_copies(n - 1))
    arrived(x_copies(n))
    arrived(z_copies(n))

    def last(c):
        sent(y_copies(n - 1, c))
        for k in range(LINES):
            for y in range(1, ny - 1):
                line_stats(one_line(n, y, c * LINES + k), c, k, y)
        arrived(y_copies(n, c))
        for k in range(LINES):
            for y in (0, ny - 1):
                line_stats(one_line(n, y, c * LINES + k), c, k, y)
        start(stat_copies(c))

    each(pieces, last)

    sent(x_copies(0))
    sent(x_copies(n))
    for m in range(STEPS):
        sent(z_copies(m))

    def drain(c):
        sent(y_copies(0, c))
        sent(y_copies(n, c))
        sent(stat_copies(c))
        arrived(stat_copies(c))

    each(pieces, drain)


def finish_kernel(field, stats, anomaly, field_end, held, sems):
    slabs, pieces, _, rows, _ = stats.shape
    ny, nx, nz, _ = field_end.shape
    whole = [
        pltpu.make_async_copy(field.at[y + 1, pl.ds(1, nx)], field_end.at[y], sems.at[y]) for y in range(ny)
    ]
    for copy in whole:
        copy.start()

    def copy_of(c):
        lines = pl.ds(c * LINES, LINES)
        return pltpu.make_async_copy(held.at[:, lines], anomaly.at[:, lines], sems.at[ny + c])

    def piece(c, carry):
        means = [stats[d, c, 0] for d in range(slabs)]
        mean = sum(means[1:], means[0]) * (1.0 / slabs)
        spread = stats[0, c, 1]
        for d in range(1, slabs):
            spread = spread + stats[d, c, 1]
        for other in means:
            spread = spread + (other - mean) * (other - mean) * float(nz)
        scale = lax.rsqrt(spread * (1.0 / (nz * slabs)) + EPS)
        for k in range(LINES):
            for y in range(ny):
                r = k * ny + y
                i = c * LINES + k
                held[y, i] = (field[y + 1, i + 1] - mean[r:r + 1]) * scale[r:r + 1]
        copy_of(c).start()
        return carry

    lax.fori_loop(0, pieces, piece, 0)
    for copy in whole:
        copy.wait()
    lax.fori_loop(0, pieces, lambda c, carry: (copy_of(c).wait(), carry)[1], 0)


def per_device(field, mobility, source):
    ny, nx, nz, levels = field.shape
    f32 = jnp.float32
    pieces = nx // LINES
    slabs = lax.axis_size("slabs")
    any_space = pl.BlockSpec(memory_space=pl.ANY)
    vmem = pl.BlockSpec(memory_space=pltpu.VMEM)
    padded = (ny + 2, nx + 2, nz, levels)
    faces = (STEPS, ny, nx, levels)
    end, stats = pl.pallas_call(
        steps_kernel,
        out_shape=(pltpu.VMEM(padded, f32), pltpu.VMEM((slabs, pieces, 2, LINES * ny, levels), f32)),
        in_specs=[any_space] * 3,
        out_specs=(vmem, vmem),
        scratch_shapes=[
            pltpu.VMEM(padded, f32),
            pltpu.VMEM(field.shape, f32),
            pltpu.VMEM(field.shape, f32),
            pltpu.VMEM(faces, f32),
            pltpu.VMEM(faces, f32),
            pltpu.VMEM((STEPS, 2, ny, nx, levels), f32),
            DMA((STEPS, 2, pieces)),
            DMA((STEPS, 2, pieces)),
            DMA((STEPS, 2)),
            DMA((STEPS, 2)),
            DMA((STEPS, 2)),
            DMA((STEPS, 2)),
            DMA((slabs - 1, pieces)),
            DMA((slabs - 1, pieces)),
            DMA((3,)),
        ],
        name="steps",
        compiler_params=pltpu.CompilerParams(
            collective_id=0, has_side_effects=True, vmem_limit_bytes=46 * 2**20
        ),
    )(field, mobility, source)
    shape = jax.ShapeDtypeStruct(field.shape, f32)
    return pl.pallas_call(
        finish_kernel,
        out_shape=(shape, shape),
        in_specs=[vmem, vmem],
        out_specs=(any_space, any_space),
        scratch_shapes=[pltpu.VMEM(field.shape, f32), DMA((ny + pieces,))],
        name="finish",
        compiler_params=pltpu.CompilerParams(vmem_limit_bytes=24 * 2**20),
    )(end, stats)


def solution(mesh):
    spec = P("rows", "cols", "slabs", None)
    return jax.shard_map(
        per_device, mesh=mesh, in_specs=(spec,) * 3, out_specs=(spec, spec), check_vma=False
    )
```

```python
import jax
import jax.numpy as jnp
from jax import lax
from jax.experimental import pallas as pl
from jax.experimental.pallas import tpu as pltpu
from jax.sharding import PartitionSpec as P

STEPS = 3
LINES = (4, 4, 4)
L = LINES[-1]
LEAVE = (7, 4)
HOLD = 1
EPS = 1e-4
MESH = pl.DeviceIdType.MESH
DMA = pltpu.SemaphoreType.DMA


def ring(axis, by):
    size = lax.axis_size(axis)
    return {axis: lax.rem(lax.axis_index(axis) + by % size, size)}


def remote(src, dst, send, recv, to):
    return pltpu.make_async_remote_copy(
        src_ref=src, dst_ref=dst, send_sem=send, recv_sem=recv, device_id=to, device_id_type=MESH
    )


def start(copies):
    for copy in copies:
        copy.start()


def wait(copies):
    for copy in copies:
        copy.wait()


def arrived(copies):
    for copy in copies:
        copy.wait_recv()


def sent(copies):
    for copy in copies:
        copy.wait_send()


def each(first, end, body):
    def step(i, carry):
        body(i)
        return carry

    lax.fori_loop(first, end, step, 0)


def leaving():
    return LEAVE[0] + (LEAVE[1] - LEAVE[0]) * lax.rem(lax.axis_index("cols"), 2)


def greet(peers):
    barrier = pltpu.get_barrier_semaphore()
    for peer in peers:
        pl.semaphore_signal(barrier, inc=1, device_id=peer, device_id_type=MESH)
    return lambda: pl.semaphore_wait(barrier, len(peers))


def others():
    return [ring("slabs", d) for d in range(1, lax.axis_size("slabs"))]


def next_value(middle, below, above, left, right, low_row, high_row, mobility, source):
    nz = middle.shape[0]
    row = lax.broadcasted_iota(jnp.int32, middle.shape, 0)
    low = jnp.where(row == 0, low_row, pltpu.roll(middle, 1, 0))
    high = jnp.where(row == nz - 1, high_row, pltpu.roll(middle, nz - 1, 0))
    return middle + mobility * (below + above + left + right + low + high - 6.0 * middle) + source


def line_stats(stats, value, c, r):
    nz = value.shape[0]
    mean = jnp.sum(value, axis=0, keepdims=True) * (1.0 / nz)
    centred = value - mean
    stats[0, c, 0, pl.ds(r, 1)] = mean
    stats[0, c, 1, pl.ds(r, 1)] = jnp.sum(centred * centred, axis=0, keepdims=True)


def stat_copies(stats, s_send, s_recv, c):
    return [
        remote(stats.at[0, c], stats.at[d, c], s_send.at[d - 1, c], s_recv.at[d - 1, c], ring("slabs", d))
        for d in range(1, lax.axis_size("slabs"))
    ]


def first_kernel(
    field, mobility, source, odd, even, z_end, stats,
    mob, src, z_in, z_out,
    y_send, y_recv, x_send, x_recv, z_send, z_recv, s_send, s_recv, local,
):
    ny, nx, nz, _ = field.shape
    pieces = [nx // lines for lines in LINES]
    leave = leaving()

    def load(y, planes, first, lines, sem):
        return pltpu.make_async_copy(
            field.at[pl.ds(y, planes), pl.ds(first, lines)],
            even.at[pl.ds(y + 1, planes), pl.ds(first + 1, lines)],
            local.at[sem],
        )

    ahead = [load(0, 1, 0, LINES[0], 0), load(ny - 1, 1, 0, LINES[0], 1)]
    loads = [
        load(0, 1, LINES[0], nx - LINES[0], 2),
        load(ny - 1, 1, LINES[0], nx - LINES[0], 3),
        load(1, ny - 2, 0, nx, 4),
    ]
    more = [
        pltpu.make_async_copy(mobility, mob, local.at[5]),
        pltpu.make_async_copy(source, src, local.at[6]),
    ]
    met = greet([ring("rows", 1), ring("rows", -1), ring("cols", 1), ring("cols", -1)] + others())
    start(ahead + loads + more)
    wait(ahead)
    met()

    def y_copies(n, c):
        buf = odd if n % 2 else even
        lines = pl.ds(1 + c * LINES[n], LINES[n])
        if n or (isinstance(c, int) and c == 0):
            first, last = buf.at[1, lines], buf.at[ny, lines]
        else:
            here = pl.ds(c * LINES[n], LINES[n])
            first, last = field.at[0, here], field.at[ny - 1, here]
        return (
            remote(last, buf.at[0, lines], y_send.at[n, 0, c], y_recv.at[n, 0, c], ring("rows", 1)),
            remote(first, buf.at[ny + 1, lines], y_send.at[n, 1, c], y_recv.at[n, 1, c], ring("rows", -1)),
        )

    def x_copies(n):
        buf = odd if n % 2 else even
        planes = pl.ds(1, ny)
        if n:
            first, last = buf.at[planes, 1], buf.at[planes, nx]
        else:
            first, last = field.at[:, 0], field.at[:, nx - 1]
        return (
            remote(last, buf.at[planes, 0], x_send.at[n, 0], x_recv.at[n, 0], ring("cols", 1)),
            remote(first, buf.at[planes, nx + 1], x_send.at[n, 1], x_recv.at[n, 1], ring("cols", -1)),
        )

    def z_faces(n):
        return z_in.at[n] if n + 1 < STEPS else z_end

    def z_copies(n):
        return (
            remote(z_out.at[n, 0], z_faces(n).at[0], z_send.at[n, 0], z_recv.at[n, 0], ring("slabs", 1)),
            remote(z_out.at[n, 1], z_faces(n).at[1], z_send.at[n, 1], z_recv.at[n, 1], ring("slabs", -1)),
        )

    start(y_copies(0, 0))
    each(1, pieces[0], lambda c: start(y_copies(0, c)))
    start(x_copies(0))
    wait(loads)

    def pack(i):
        for y in range(ny):
            z_out[0, 0, y, pl.ds(i, 1)] = even[y + 1, i + 1, pl.ds(nz - 1, 1)]
            z_out[0, 1, y, pl.ds(i, 1)] = even[y + 1, i + 1, pl.ds(0, 1)]

    each(0, nx, pack)
    start(z_copies(0))
    wait(more)

    def one_line(n, y, i):
        old, new = (odd, even) if n % 2 else (even, odd)
        faces = z_faces(n)
        value = next_value(
            old[y + 1, i + 1], old[y, i + 1], old[y + 2, i + 1], old[y + 1, i], old[y + 1, i + 2],
            faces[0, y, pl.ds(i, 1)], faces[1, y, pl.ds(i, 1)], mob[y, i], src[y, i],
        )
        new[y + 1, i + 1] = value
        if n + 1 < STEPS:
            z_out[n + 1, 0, y, pl.ds(i, 1)] = value[nz - 1:]
            z_out[n + 1, 1, y, pl.ds(i, 1)] = value[:1]
        return value

    def send_piece(n, c):
        if n + 1 < STEPS:
            start(y_copies(n, c))
            return
        parts = LINES[n - 1] // LINES[n]
        for part in range(parts):

            @pl.when(c * parts + part < leave)
            def _():
                start(y_copies(n, c * parts + part))

    for n in range(STEPS - 1):
        if n == 1:
            sent(y_copies(0, 0))
        arrived(x_copies(n))
        arrived(z_copies(n))

        def inner(i):
            for y in range(1, ny - 1):
                one_line(n, y, i)

        def outer(c):
            arrived(y_copies(n, c))

            def line(k):
                for y in (0, ny - 1):
                    one_line(n, y, c * LINES[n] + k)

            each(0, LINES[n], line)

        def outer_and_send(c):
            outer(c)
            send_piece(n + 1, c - 1)

        each(0, nx, inner)
        outer(0)
        each(1, pieces[n], outer_and_send)
        start(x_copies(n + 1))
        start(z_copies(n + 1))
        send_piece(n + 1, pieces[n] - 1)

    n = STEPS - 1
    each(0, pieces[n - 1], lambda c: sent(y_copies(n - 1, c)))
    sent(x_copies(n - 1))
    arrived(x_copies(n))
    arrived(z_copies(n))

    def last(c):
        for k in range(L):
            for y in range(1, ny - 1):
                line_stats(stats, one_line(n, y, c * L + k), c, k * ny + y)
        arrived(y_copies(n, c))
        for k in range(L):
            for y in (0, ny - 1):
                line_stats(stats, one_line(n, y, c * L + k), c, k * ny + y)
        start(stat_copies(stats, s_send, s_recv, c))

    each(0, leave - HOLD, last)
    each(leave - HOLD, leave, lambda c: arrived(y_copies(n, c)))
    each(0, leave, lambda c: sent(y_copies(n, c)))
    each(1, pieces[0], lambda c: sent(y_copies(0, c)))
    sent(x_copies(0))
    sent(x_copies(n))
    for m in range(STEPS):
        sent(z_copies(m))

    def drain(c):
        sent(stat_copies(stats, s_send, s_recv, c))
        arrived(stat_copies(stats, s_send, s_recv, c))

    each(0, leave - HOLD, drain)


def second_kernel(
    even, z_end, mobility, source, after, rest, stats,
    mob, src, halo, y_send, y_recv, s_send, s_recv, local,
):
    ny, nx, nz, _ = mobility.shape
    pieces = nx // L
    leave = leaving()
    begin = leave - HOLD

    def loads(c):
        there, here = pl.ds(c * L, L), pl.ds((c - begin) * L, L)
        return (
            pltpu.make_async_copy(mobility.at[:, there], mob.at[:, here], local.at[0, c - begin]),
            pltpu.make_async_copy(source.at[:, there], src.at[:, here], local.at[1, c - begin]),
        )

    def y_copies(c):
        lines, landing = pl.ds(1 + c * L, L), pl.ds((c - leave) * L, L)
        p = c - leave
        return (
            remote(even.at[ny, lines], halo.at[0, landing], y_send.at[0, p], y_recv.at[0, p], ring("rows", 1)),
            remote(even.at[1, lines], halo.at[1, landing], y_send.at[1, p], y_recv.at[1, p], ring("rows", -1)),
        )

    def my_stats(c):
        return stat_copies(stats, s_send, s_recv, c - begin)

    met = greet([ring("rows", 1), ring("rows", -1)] + others())
    each(begin, pieces, lambda c: start(loads(c)))
    met()
    each(leave, pieces, lambda c: start(y_copies(c)))

    def one_line(c, k, y, landed):
        i = c * L + k
        r = (c - begin) * L + k
        below = halo[0, (c - leave) * L + k] if landed and y == 0 else even[y, i + 1]
        above = halo[1, (c - leave) * L + k] if landed and y == ny - 1 else even[y + 2, i + 1]
        value = next_value(
            even[y + 1, i + 1], below, above, even[y + 1, i], even[y + 1, i + 2],
            z_end[0, y, pl.ds(i, 1)], z_end[1, y, pl.ds(i, 1)], mob[y, r], src[y, r],
        )
        rest[y, r] = value
        line_stats(stats, value, c - begin, k * ny + y)

    def inner(c, landed):
        wait(loads(c))
        for k in range(L):
            for y in range(1, ny - 1):
                one_line(c, k, y, landed)

    def outer(c, landed):
        for k in range(L):
            for y in (0, ny - 1):
                one_line(c, k, y, landed)
        start(my_stats(c))

    def held(c):
        inner(c, False)
        outer(c, False)

    def moved(c):
        inner(c, True)
        arrived(y_copies(c))
        outer(c, True)

    each(begin, leave, held)
    each(leave, pieces, moved)
    each(leave, pieces, lambda c: sent(y_copies(c)))

    def drain(c):
        sent(my_stats(c))
        arrived(my_stats(c))

    each(begin, pieces, drain)


def write_pieces(first, end, stats_of, value_of, block_of, anomaly, field_end, held, sems):
    ny, _, nz, _ = field_end.shape

    def field_copy(c):
        return pltpu.make_async_copy(block_of(c), field_end.at[:, pl.ds(c * L, L)], sems.at[0, c])

    def anomaly_copy(c):
        lines = pl.ds(c * L, L)
        return pltpu.make_async_copy(held.at[:, lines], anomaly.at[:, lines], sems.at[1, c])

    def piece(c):
        stats = stats_of(c)
        slabs = len(stats)
        mean = sum((a for a, _ in stats[1:]), stats[0][0]) * (1.0 / slabs)
        spread = sum((b for _, b in stats[1:]), stats[0][1])
        for a, _ in stats:
            spread = spread + (a - mean) * (a - mean) * float(nz)
        scale = lax.rsqrt(spread * (1.0 / (nz * slabs)) + EPS)
        for k in range(L):
            for y in range(ny):
                r = k * ny + y
                held[y, c * L + k] = (value_of(c, k, y) - mean[r:r + 1]) * scale[r:r + 1]
        anomaly_copy(c).start()

    each(first, end, lambda c: field_copy(c).start())
    each(first, end, piece)

    def done(c):
        field_copy(c).wait()
        anomaly_copy(c).wait()

    each(first, end, done)


def first_write(odd, stats, anomaly, field_end, after, held, sems):
    ny = field_end.shape[0]
    slabs = stats.shape[0]
    write_pieces(
        0, leaving() - HOLD,
        lambda c: [(stats[d, c, 0], stats[d, c, 1]) for d in range(slabs)],
        lambda c, k, y: odd[y + 1, c * L + k + 1],
        lambda c: odd.at[pl.ds(1, ny), pl.ds(c * L + 1, L)],
        anomaly, field_end, held, sems,
    )
    after[...] = jnp.zeros_like(after)


def second_write(rest, stats, _a, _f, anomaly, field_end, held, sems):
    slabs = stats.shape[0]
    begin = leaving() - HOLD
    write_pieces(
        begin, field_end.shape[1] // L,
        lambda c: [(stats[d, c - begin, 0], stats[d, c - begin, 1]) for d in range(slabs)],
        lambda c, k, y: rest[y, (c - begin) * L + k],
        lambda c: rest.at[:, pl.ds((c - begin) * L, L)],
        anomaly, field_end, held, sems,
    )


def near(x):
    return pltpu.with_memory_space_constraint(x, pltpu.VMEM)


def far(x):
    return pltpu.with_memory_space_constraint(x, pltpu.HBM)


def per_device(field, mobility, source):
    ny, nx, nz, levels = field.shape
    f32 = jnp.float32
    pieces = nx // L
    most = nx // min(LINES)
    slabs = lax.axis_size("slabs")
    any_space = pl.BlockSpec(memory_space=pl.ANY)
    vmem = pl.BlockSpec(memory_space=pltpu.VMEM)
    padded = (ny + 2, nx + 2, nz, levels)
    faces = (2, ny, nx, levels)
    left = pieces - min(LEAVE) + HOLD
    coming = pieces - min(LEAVE)
    odd, even, z_end, stats = pl.pallas_call(
        first_kernel,
        out_shape=(
            pltpu.VMEM(padded, f32),
            pltpu.VMEM(padded, f32),
            pltpu.VMEM(faces, f32),
            pltpu.VMEM((slabs, pieces, 2, L * ny, levels), f32),
        ),
        in_specs=[any_space] * 3,
        out_specs=(vmem,) * 4,
        scratch_shapes=[
            pltpu.VMEM(field.shape, f32),
            pltpu.VMEM(field.shape, f32),
            pltpu.VMEM((STEPS - 1, *faces), f32),
            pltpu.VMEM((STEPS, *faces), f32),
            DMA((STEPS, 2, most)),
            DMA((STEPS, 2, most)),
            DMA((STEPS, 2)),
            DMA((STEPS, 2)),
            DMA((STEPS, 2)),
            DMA((STEPS, 2)),
            DMA((slabs - 1, pieces)),
            DMA((slabs - 1, pieces)),
            DMA((7,)),
        ],
        name="steps",
        compiler_params=pltpu.CompilerParams(
            collective_id=0, has_side_effects=True, vmem_limit_bytes=22 * 2**20
        ),
    )(field, mobility, source)
    shape = jax.ShapeDtypeStruct(field.shape, f32)
    writing = dict(
        scratch_shapes=[pltpu.VMEM(field.shape, f32), DMA((2, pieces))],
        compiler_params=pltpu.CompilerParams(vmem_limit_bytes=12 * 2**20),
    )
    anomaly, field_end, after = pl.pallas_call(
        first_write,
        out_shape=(shape, shape, jax.ShapeDtypeStruct((8, levels), f32)),
        in_specs=[vmem, vmem],
        out_specs=(any_space, any_space, vmem),
        name="write",
        **writing,
    )(near(odd), near(stats))
    rest, stats = pl.pallas_call(
        second_kernel,
        out_shape=(
            pltpu.VMEM((ny, left * L, nz, levels), f32),
            pltpu.VMEM((slabs, left, 2, L * ny, levels), f32),
        ),
        in_specs=[vmem, vmem, any_space, any_space, any_space],
        out_specs=(vmem, vmem),
        scratch_shapes=[
            pltpu.VMEM((ny, left * L, nz, levels), f32),
            pltpu.VMEM((ny, left * L, nz, levels), f32),
            pltpu.VMEM((2, coming * L, nz, levels), f32),
            DMA((2, coming)),
            DMA((2, coming)),
            DMA((slabs - 1, left)),
            DMA((slabs - 1, left)),
            DMA((2, left)),
        ],
        name="rest",
        compiler_params=pltpu.CompilerParams(
            collective_id=1, has_side_effects=True, vmem_limit_bytes=16 * 2**20
        ),
    )(near(even), near(z_end), far(mobility), far(source), after)
    return pl.pallas_call(
        second_write,
        out_shape=(shape, shape),
        in_specs=[vmem, vmem, any_space, any_space],
        out_specs=(any_space, any_space),
        input_output_aliases={2: 0, 3: 1},
        name="write_rest",
        **writing,
    )(near(rest), near(stats), anomaly, field_end)


def solution(mesh):
    spec = P("rows", "cols", "slabs", None)
    return jax.shard_map(
        per_device, mesh=mesh, in_specs=(spec,) * 3, out_specs=(spec, spec), check_vma=False
    )
```

```python
import jax
import jax.numpy as jnp
from jax import lax
from jax.experimental import pallas as pl
from jax.experimental.pallas import tpu as pltpu
from jax.sharding import PartitionSpec as P

STEPS = 3
LINES = (4, 4, 4)
L = LINES[-1]
LEAVE = (7, 3)
HOLD = (1, 1)
INNER = (1, 2)
EPS = 1e-4
MESH = pl.DeviceIdType.MESH
DMA = pltpu.SemaphoreType.DMA


def ring(axis, by):
    size = lax.axis_size(axis)
    return {axis: lax.rem(lax.axis_index(axis) + by % size, size)}


def remote(src, dst, send, recv, to):
    return pltpu.make_async_remote_copy(
        src_ref=src, dst_ref=dst, send_sem=send, recv_sem=recv, device_id=to, device_id_type=MESH
    )


def start(copies):
    for copy in copies:
        copy.start()


def wait(copies):
    for copy in copies:
        copy.wait()


def arrived(copies):
    for copy in copies:
        copy.wait_recv()


def sent(copies):
    for copy in copies:
        copy.wait_send()


def each(first, end, body):
    def step(i, carry):
        body(i)
        return carry

    lax.fori_loop(first, end, step, 0)


def by_core(values):
    return values[0] + (values[1] - values[0]) * lax.rem(lax.axis_index("cols"), 2)


def leaving():
    return by_core(LEAVE)


def beginning():
    return by_core([leave - hold for leave, hold in zip(LEAVE, HOLD)])


def greet(peers):
    barrier = pltpu.get_barrier_semaphore()
    for peer in peers:
        pl.semaphore_signal(barrier, inc=1, device_id=peer, device_id_type=MESH)
    return lambda: pl.semaphore_wait(barrier, len(peers))


def others():
    return [ring("slabs", d) for d in range(1, lax.axis_size("slabs"))]


def next_value(middle, below, above, left, right, low_row, high_row, mobility, source):
    nz = middle.shape[0]
    row = lax.broadcasted_iota(jnp.int32, middle.shape, 0)
    low = jnp.where(row == 0, low_row, pltpu.roll(middle, 1, 0))
    high = jnp.where(row == nz - 1, high_row, pltpu.roll(middle, nz - 1, 0))
    return middle + mobility * (below + above + left + right + low + high - 6.0 * middle) + source


def line_stats(stats, value, c, r):
    nz = value.shape[0]
    mean = jnp.sum(value, axis=0, keepdims=True) * (1.0 / nz)
    centred = value - mean
    stats[0, c, 0, pl.ds(r, 1)] = mean
    stats[0, c, 1, pl.ds(r, 1)] = jnp.sum(centred * centred, axis=0, keepdims=True)


def stat_copies(stats, s_send, s_recv, c):
    return [
        remote(stats.at[0, c], stats.at[d, c], s_send.at[d - 1, c], s_recv.at[d - 1, c], ring("slabs", d))
        for d in range(1, lax.axis_size("slabs"))
    ]


def first_kernel(
    field, mobility, source, odd, even, z_end, inner_stats, outer_stats,
    mob, src, z_in, z_out,
    y_send, y_recv, x_send, x_recv, z_send, z_recv, i_send, i_recv, s_send, s_recv, local,
):
    ny, nx, nz, _ = field.shape
    pieces = [nx // lines for lines in LINES]
    leave = leaving()
    begin = beginning()

    def load(y, planes, first, lines, sem):
        return pltpu.make_async_copy(
            field.at[pl.ds(y, planes), pl.ds(first, lines)],
            even.at[pl.ds(y + 1, planes), pl.ds(first + 1, lines)],
            local.at[sem],
        )

    ahead = [load(0, 1, 0, LINES[0], 0), load(ny - 1, 1, 0, LINES[0], 1)]
    loads = [
        load(0, 1, LINES[0], nx - LINES[0], 2),
        load(ny - 1, 1, LINES[0], nx - LINES[0], 3),
        load(1, ny - 2, 0, nx, 4),
    ]
    more = [
        pltpu.make_async_copy(mobility, mob, local.at[5]),
        pltpu.make_async_copy(source, src, local.at[6]),
    ]
    met = greet([ring("rows", 1), ring("rows", -1), ring("cols", 1), ring("cols", -1)] + others())
    start(ahead + loads + more)
    wait(ahead)
    met()

    def y_copies(n, c):
        buf = odd if n % 2 else even
        lines = pl.ds(1 + c * LINES[n], LINES[n])
        if n or (isinstance(c, int) and c == 0):
            first, last = buf.at[1, lines], buf.at[ny, lines]
        else:
            here = pl.ds(c * LINES[n], LINES[n])
            first, last = field.at[0, here], field.at[ny - 1, here]
        return (
            remote(last, buf.at[0, lines], y_send.at[n, 0, c], y_recv.at[n, 0, c], ring("rows", 1)),
            remote(first, buf.at[ny + 1, lines], y_send.at[n, 1, c], y_recv.at[n, 1, c], ring("rows", -1)),
        )

    def x_copies(n):
        buf = odd if n % 2 else even
        planes = pl.ds(1, ny)
        if n:
            first, last = buf.at[planes, 1], buf.at[planes, nx]
        else:
            first, last = field.at[:, 0], field.at[:, nx - 1]
        return (
            remote(last, buf.at[planes, 0], x_send.at[n, 0], x_recv.at[n, 0], ring("cols", 1)),
            remote(first, buf.at[planes, nx + 1], x_send.at[n, 1], x_recv.at[n, 1], ring("cols", -1)),
        )

    def z_faces(n):
        return z_in.at[n] if n + 1 < STEPS else z_end

    def z_copies(n):
        return (
            remote(z_out.at[n, 0], z_faces(n).at[0], z_send.at[n, 0], z_recv.at[n, 0], ring("slabs", 1)),
            remote(z_out.at[n, 1], z_faces(n).at[1], z_send.at[n, 1], z_recv.at[n, 1], ring("slabs", -1)),
        )

    start(y_copies(0, 0))
    each(1, pieces[0], lambda c: start(y_copies(0, c)))
    start(x_copies(0))
    wait(loads)

    def pack(i):
        for y in range(ny):
            z_out[0, 0, y, pl.ds(i, 1)] = even[y + 1, i + 1, pl.ds(nz - 1, 1)]
            z_out[0, 1, y, pl.ds(i, 1)] = even[y + 1, i + 1, pl.ds(0, 1)]

    each(0, nx, pack)
    start(z_copies(0))
    wait(more)

    def one_line(n, y, i):
        old, new = (odd, even) if n % 2 else (even, odd)
        faces = z_faces(n)
        value = next_value(
            old[y + 1, i + 1], old[y, i + 1], old[y + 2, i + 1], old[y + 1, i], old[y + 1, i + 2],
            faces[0, y, pl.ds(i, 1)], faces[1, y, pl.ds(i, 1)], mob[y, i], src[y, i],
        )
        new[y + 1, i + 1] = value
        if n + 1 < STEPS:
            z_out[n + 1, 0, y, pl.ds(i, 1)] = value[nz - 1:]
            z_out[n + 1, 1, y, pl.ds(i, 1)] = value[:1]
        return value

    def send_piece(n, c):
        if n + 1 < STEPS:
            start(y_copies(n, c))
            return
        parts = LINES[n - 1] // LINES[n]
        for part in range(parts):

            @pl.when(c * parts + part < leave)
            def _():
                start(y_copies(n, c * parts + part))

    for n in range(STEPS - 1):
        if n == 1:
            sent(y_copies(0, 0))
        arrived(x_copies(n))
        arrived(z_copies(n))

        def inner(i):
            for y in range(1, ny - 1):
                one_line(n, y, i)

        def outer(c):
            arrived(y_copies(n, c))

            def line(k):
                for y in (0, ny - 1):
                    one_line(n, y, c * LINES[n] + k)

            each(0, LINES[n], line)

        def outer_and_send(c):
            outer(c)
            send_piece(n + 1, c - 1)

        each(0, nx, inner)
        outer(0)
        each(1, pieces[n], outer_and_send)
        start(x_copies(n + 1))
        start(z_copies(n + 1))
        send_piece(n + 1, pieces[n] - 1)

    n = STEPS - 1
    each(0, pieces[n - 1], lambda c: sent(y_copies(n - 1, c)))
    sent(x_copies(n - 1))
    arrived(x_copies(n))
    arrived(z_copies(n))

    def all_inner_stats():
        return [
            remote(inner_stats.at[0], inner_stats.at[d], i_send.at[d - 1], i_recv.at[d - 1], ring("slabs", d))
            for d in range(1, lax.axis_size("slabs"))
        ]

    def inner_piece(c):
        for k in range(L):
            for p, y in enumerate(INNER):
                line_stats(inner_stats, one_line(n, y, c * L + k), c, 2 * k + p)

    def last(c):
        arrived(y_copies(n, c))
        for k in range(L):
            for p, y in enumerate((0, ny - 1)):
                line_stats(outer_stats, one_line(n, y, c * L + k), c, 2 * k + p)
        start(stat_copies(outer_stats, s_send, s_recv, c))

    each(0, pieces[n], inner_piece)
    start(all_inner_stats())
    each(0, begin, last)
    each(begin, leave, lambda c: arrived(y_copies(n, c)))
    each(0, leave, lambda c: sent(y_copies(n, c)))
    each(1, pieces[0], lambda c: sent(y_copies(0, c)))
    sent(x_copies(0))
    sent(x_copies(n))
    for m in range(STEPS):
        sent(z_copies(m))

    def drain(c):
        sent(stat_copies(outer_stats, s_send, s_recv, c))
        arrived(stat_copies(outer_stats, s_send, s_recv, c))

    each(0, begin, drain)
    sent(all_inner_stats())
    arrived(all_inner_stats())


def second_kernel(
    even, z_end, mobility, source, after, rest, stats,
    mob, src, halo, y_send, y_recv, s_send, s_recv, local,
):
    ny, nx, nz, _ = mobility.shape
    pieces = nx // L
    leave = leaving()
    begin = beginning()

    def loads(c):
        there, here = pl.ds(c * L, L), pl.ds((c - begin) * L, L)
        return [
            pltpu.make_async_copy(whole.at[y, there], part.at[p, here], local.at[q, p, c - begin])
            for q, (whole, part) in enumerate(((mobility, mob), (source, src)))
            for p, y in enumerate((0, ny - 1))
        ]

    def y_copies(c):
        lines, landing = pl.ds(1 + c * L, L), pl.ds((c - leave) * L, L)
        p = c - leave
        return (
            remote(even.at[ny, lines], halo.at[0, landing], y_send.at[0, p], y_recv.at[0, p], ring("rows", 1)),
            remote(even.at[1, lines], halo.at[1, landing], y_send.at[1, p], y_recv.at[1, p], ring("rows", -1)),
        )

    def my_stats(c):
        return stat_copies(stats, s_send, s_recv, c - begin)

    @pl.when(begin < pieces)
    def _():
        met = greet([ring("rows", 1), ring("rows", -1)] + others())
        each(begin, pieces, lambda c: start(loads(c)))
        met()
        each(leave, pieces, lambda c: start(y_copies(c)))

        def piece(c, landed):
            for k in range(L):
                i = c * L + k
                r = (c - begin) * L + k
                for p, y in enumerate((0, ny - 1)):
                    below = halo[0, (c - leave) * L + k] if landed and p == 0 else even[y, i + 1]
                    above = halo[1, (c - leave) * L + k] if landed and p == 1 else even[y + 2, i + 1]
                    value = next_value(
                        even[y + 1, i + 1], below, above, even[y + 1, i], even[y + 1, i + 2],
                        z_end[0, y, pl.ds(i, 1)], z_end[1, y, pl.ds(i, 1)], mob[p, r], src[p, r],
                    )
                    rest[p, r] = value
                    line_stats(stats, value, c - begin, 2 * k + p)
            start(my_stats(c))

        def held(c):
            wait(loads(c))
            piece(c, False)

        def moved(c):
            wait(loads(c))
            arrived(y_copies(c))
            piece(c, True)

        each(begin, leave, held)
        each(leave, pieces, moved)
        each(leave, pieces, lambda c: sent(y_copies(c)))

        def drain(c):
            sent(my_stats(c))
            arrived(my_stats(c))

        each(begin, pieces, drain)


def write_planes(first, end, planes, stats, value_of, block_of, at, anomaly, field_end, held, sems):
    _, _, nz, _ = field_end.shape
    slabs = stats.shape[0]

    def field_copies(c):
        lines = pl.ds(c * L, L)
        return [pltpu.make_async_copy(block_of(c, p), field_end.at[y, lines], sems.at[0, y, c]) for p, y in enumerate(planes)]

    def anomaly_copies(c):
        lines = pl.ds(c * L, L)
        return [pltpu.make_async_copy(held.at[y, lines], anomaly.at[y, lines], sems.at[1, y, c]) for y in planes]

    def piece(c):
        means = [stats[d, c - at, 0] for d in range(slabs)]
        mean = sum(means[1:], means[0]) * (1.0 / slabs)
        spread = stats[0, c - at, 1]
        for d in range(1, slabs):
            spread = spread + stats[d, c - at, 1]
        for other in means:
            spread = spread + (other - mean) * (other - mean) * float(nz)
        scale = lax.rsqrt(spread * (1.0 / (nz * slabs)) + EPS)
        for k in range(L):
            for p, y in enumerate(planes):
                r = 2 * k + p
                held[y, c * L + k] = (value_of(c, k, p) - mean[r:r + 1]) * scale[r:r + 1]
        start(anomaly_copies(c))

    def done(c):
        wait(field_copies(c))
        wait(anomaly_copies(c))

    return (
        lambda: each(first, end, lambda c: start(field_copies(c))),
        lambda: each(first, end, piece),
        lambda: each(first, end, done),
    )


def first_write(odd, inner_stats, outer_stats, anomaly, field_end, after, held, sems):
    ny, nx = field_end.shape[:2]

    def from_odd(first, end, planes, stats):
        return write_planes(
            first, end, planes, stats,
            lambda c, k, p: odd[planes[p] + 1, c * L + k + 1],
            lambda c, p: odd.at[planes[p] + 1, pl.ds(c * L + 1, L)],
            0, anomaly, field_end, held, sems,
        )

    parts = (from_odd(0, nx // L, INNER, inner_stats), from_odd(0, beginning(), (0, ny - 1), outer_stats))
    for phase in zip(*parts):
        for run in phase:
            run()
    after[...] = jnp.zeros_like(after)


def second_write(rest, stats, _a, _f, anomaly, field_end, held, sems):
    ny, nx = field_end.shape[:2]
    begin = beginning()
    for run in write_planes(
        begin, nx // L, (0, ny - 1), stats,
        lambda c, k, p: rest[p, (c - begin) * L + k],
        lambda c, p: rest.at[p, pl.ds((c - begin) * L, L)],
        begin, anomaly, field_end, held, sems,
    ):
        run()


def near(x):
    return pltpu.with_memory_space_constraint(x, pltpu.VMEM)


def far(x):
    return pltpu.with_memory_space_constraint(x, pltpu.HBM)


def per_device(field, mobility, source):
    ny, nx, nz, levels = field.shape
    f32 = jnp.float32
    pieces = nx // L
    most = nx // min(LINES)
    slabs = lax.axis_size("slabs")
    any_space = pl.BlockSpec(memory_space=pl.ANY)
    vmem = pl.BlockSpec(memory_space=pltpu.VMEM)
    padded = (ny + 2, nx + 2, nz, levels)
    faces = (2, ny, nx, levels)
    left = pieces - min(leave - hold for leave, hold in zip(LEAVE, HOLD))
    coming = pieces - min(LEAVE)
    odd, even, z_end, inner_stats, outer_stats = pl.pallas_call(
        first_kernel,
        out_shape=(
            pltpu.VMEM(padded, f32),
            pltpu.VMEM(padded, f32),
            pltpu.VMEM(faces, f32),
            pltpu.VMEM((slabs, pieces, 2, L * 2, levels), f32),
            pltpu.VMEM((slabs, pieces, 2, L * 2, levels), f32),
        ),
        in_specs=[any_space] * 3,
        out_specs=(vmem,) * 5,
        scratch_shapes=[
            pltpu.VMEM(field.shape, f32),
            pltpu.VMEM(field.shape, f32),
            pltpu.VMEM((STEPS - 1, *faces), f32),
            pltpu.VMEM((STEPS, *faces), f32),
            DMA((STEPS, 2, most)),
            DMA((STEPS, 2, most)),
            DMA((STEPS, 2)),
            DMA((STEPS, 2)),
            DMA((STEPS, 2)),
            DMA((STEPS, 2)),
            DMA((slabs - 1,)),
            DMA((slabs - 1,)),
            DMA((slabs - 1, pieces)),
            DMA((slabs - 1, pieces)),
            DMA((7,)),
        ],
        name="steps",
        compiler_params=pltpu.CompilerParams(
            collective_id=0, has_side_effects=True, vmem_limit_bytes=22 * 2**20
        ),
    )(field, mobility, source)
    shape = jax.ShapeDtypeStruct(field.shape, f32)
    writing = dict(
        scratch_shapes=[pltpu.VMEM(field.shape, f32), DMA((2, ny, pieces))],
        compiler_params=pltpu.CompilerParams(vmem_limit_bytes=12 * 2**20),
    )
    anomaly, field_end, after = pl.pallas_call(
        first_write,
        out_shape=(shape, shape, jax.ShapeDtypeStruct((8, levels), f32)),
        in_specs=[vmem, vmem, vmem],
        out_specs=(any_space, any_space, vmem),
        name="write",
        **writing,
    )(near(odd), near(inner_stats), near(outer_stats))
    rest, stats = pl.pallas_call(
        second_kernel,
        out_shape=(
            pltpu.VMEM((2, left * L, nz, levels), f32),
            pltpu.VMEM((slabs, left, 2, L * 2, levels), f32),
        ),
        in_specs=[vmem, vmem, any_space, any_space, any_space],
        out_specs=(vmem, vmem),
        scratch_shapes=[
            pltpu.VMEM((2, left * L, nz, levels), f32),
            pltpu.VMEM((2, left * L, nz, levels), f32),
            pltpu.VMEM((2, coming * L, nz, levels), f32),
            DMA((2, coming)),
            DMA((2, coming)),
            DMA((slabs - 1, left)),
            DMA((slabs - 1, left)),
            DMA((2, 2, left)),
        ],
        name="rest",
        compiler_params=pltpu.CompilerParams(
            collective_id=1, has_side_effects=True, vmem_limit_bytes=16 * 2**20
        ),
    )(near(even), near(z_end), far(mobility), far(source), after)
    return pl.pallas_call(
        second_write,
        out_shape=(shape, shape),
        in_specs=[vmem, vmem, any_space, any_space],
        out_specs=(any_space, any_space),
        input_output_aliases={2: 0, 3: 1},
        name="write_rest",
        **writing,
    )(near(rest), near(stats), anomaly, field_end)


def solution(mesh):
    spec = P("rows", "cols", "slabs", None)
    return jax.shard_map(
        per_device, mesh=mesh, in_specs=(spec,) * 3, out_specs=(spec, spec), check_vma=False
    )
```

```python
import jax
import jax.numpy as jnp
from jax import lax
from jax.experimental import pallas as pl
from jax.experimental.pallas import tpu as pltpu
from jax.sharding import PartitionSpec as P

STEPS = 3
LINES = (8, 8, 4)
L = LINES[-1]
LEAVE = (7, 3)
HOLD = (1, 1)
INNER = (1, 2)
EPS = 1e-4
MESH = pl.DeviceIdType.MESH
DMA = pltpu.SemaphoreType.DMA


def ring(axis, by):
    size = lax.axis_size(axis)
    return {axis: lax.rem(lax.axis_index(axis) + by % size, size)}


def remote(src, dst, send, recv, to):
    return pltpu.make_async_remote_copy(
        src_ref=src, dst_ref=dst, send_sem=send, recv_sem=recv, device_id=to, device_id_type=MESH
    )


def start(copies):
    for copy in copies:
        copy.start()


def wait(copies):
    for copy in copies:
        copy.wait()


def arrived(copies):
    for copy in copies:
        copy.wait_recv()


def sent(copies):
    for copy in copies:
        copy.wait_send()


def each(first, end, body):
    def step(i, carry):
        body(i)
        return carry

    lax.fori_loop(first, end, step, 0)


def by_core(values):
    return values[0] + (values[1] - values[0]) * lax.rem(lax.axis_index("cols"), 2)


def leaving():
    return by_core(LEAVE)


def beginning():
    return by_core([leave - hold for leave, hold in zip(LEAVE, HOLD)])


def greet(peers):
    barrier = pltpu.get_barrier_semaphore()
    for peer in peers:
        pl.semaphore_signal(barrier, inc=1, device_id=peer, device_id_type=MESH)
    return lambda: pl.semaphore_wait(barrier, len(peers))


def others():
    return [ring("slabs", d) for d in range(1, lax.axis_size("slabs"))]


def next_value(middle, below, above, left, right, low_row, high_row, mobility, source):
    nz = middle.shape[0]
    row = lax.broadcasted_iota(jnp.int32, middle.shape, 0)
    low = jnp.where(row == 0, low_row, pltpu.roll(middle, 1, 0))
    high = jnp.where(row == nz - 1, high_row, pltpu.roll(middle, nz - 1, 0))
    return middle + mobility * (below + above + left + right + low + high - 6.0 * middle) + source


def line_stats(stats, value, c, r):
    nz = value.shape[0]
    mean = jnp.sum(value, axis=0, keepdims=True) * (1.0 / nz)
    centred = value - mean
    stats[0, c, 0, pl.ds(r, 1)] = mean
    stats[0, c, 1, pl.ds(r, 1)] = jnp.sum(centred * centred, axis=0, keepdims=True)


def stat_copies(stats, s_send, s_recv, c):
    return [
        remote(stats.at[0, c], stats.at[d, c], s_send.at[d - 1, c], s_recv.at[d - 1, c], ring("slabs", d))
        for d in range(1, lax.axis_size("slabs"))
    ]


def first_kernel(
    field, mobility, source, odd, even, z_end, inner_stats, outer_stats,
    mob, src, z_in, z_out,
    y_send, y_recv, x_send, x_recv, z_send, z_recv, i_send, i_recv, s_send, s_recv, local,
):
    ny, nx, nz, _ = field.shape
    pieces = [nx // lines for lines in LINES]
    leave = leaving()
    begin = beginning()

    def load(y, planes, first, lines, sem):
        return pltpu.make_async_copy(
            field.at[pl.ds(y, planes), pl.ds(first, lines)],
            even.at[pl.ds(y + 1, planes), pl.ds(first + 1, lines)],
            local.at[sem],
        )

    ahead = [load(0, 1, 0, LINES[0], 0), load(ny - 1, 1, 0, LINES[0], 1)]
    loads = [
        load(0, 1, LINES[0], nx - LINES[0], 2),
        load(ny - 1, 1, LINES[0], nx - LINES[0], 3),
        load(1, ny - 2, 0, nx, 4),
    ]
    more = [
        pltpu.make_async_copy(mobility, mob, local.at[5]),
        pltpu.make_async_copy(source, src, local.at[6]),
    ]
    met = greet([ring("rows", 1), ring("rows", -1), ring("cols", 1), ring("cols", -1)] + others())
    start(ahead + loads + more)
    wait(ahead)
    met()

    def y_copies(n, c):
        buf = odd if n % 2 else even
        lines = pl.ds(1 + c * LINES[n], LINES[n])
        if n or (isinstance(c, int) and c == 0):
            first, last = buf.at[1, lines], buf.at[ny, lines]
        else:
            here = pl.ds(c * LINES[n], LINES[n])
            first, last = field.at[0, here], field.at[ny - 1, here]
        return (
            remote(last, buf.at[0, lines], y_send.at[n, 0, c], y_recv.at[n, 0, c], ring("rows", 1)),
            remote(first, buf.at[ny + 1, lines], y_send.at[n, 1, c], y_recv.at[n, 1, c], ring("rows", -1)),
        )

    def x_copies(n):
        buf = odd if n % 2 else even
        planes = pl.ds(1, ny)
        if n:
            first, last = buf.at[planes, 1], buf.at[planes, nx]
        else:
            first, last = field.at[:, 0], field.at[:, nx - 1]
        return (
            remote(last, buf.at[planes, 0], x_send.at[n, 0], x_recv.at[n, 0], ring("cols", 1)),
            remote(first, buf.at[planes, nx + 1], x_send.at[n, 1], x_recv.at[n, 1], ring("cols", -1)),
        )

    def z_faces(n):
        return z_in.at[n] if n + 1 < STEPS else z_end

    def z_copies(n):
        return (
            remote(z_out.at[n, 0], z_faces(n).at[0], z_send.at[n, 0], z_recv.at[n, 0], ring("slabs", 1)),
            remote(z_out.at[n, 1], z_faces(n).at[1], z_send.at[n, 1], z_recv.at[n, 1], ring("slabs", -1)),
        )

    start(y_copies(0, 0))
    each(1, pieces[0], lambda c: start(y_copies(0, c)))
    start(x_copies(0))
    wait(loads)

    def pack(i):
        for y in range(ny):
            z_out[0, 0, y, pl.ds(i, 1)] = even[y + 1, i + 1, pl.ds(nz - 1, 1)]
            z_out[0, 1, y, pl.ds(i, 1)] = even[y + 1, i + 1, pl.ds(0, 1)]

    each(0, nx, pack)
    start(z_copies(0))
    wait(more)

    def one_line(n, y, i):
        old, new = (odd, even) if n % 2 else (even, odd)
        faces = z_faces(n)
        value = next_value(
            old[y + 1, i + 1], old[y, i + 1], old[y + 2, i + 1], old[y + 1, i], old[y + 1, i + 2],
            faces[0, y, pl.ds(i, 1)], faces[1, y, pl.ds(i, 1)], mob[y, i], src[y, i],
        )
        new[y + 1, i + 1] = value
        if n + 1 < STEPS:
            z_out[n + 1, 0, y, pl.ds(i, 1)] = value[nz - 1:]
            z_out[n + 1, 1, y, pl.ds(i, 1)] = value[:1]
        return value

    def send_piece(n, c):
        if n + 1 < STEPS:
            start(y_copies(n, c))
            return
        parts = LINES[n - 1] // LINES[n]
        for part in range(parts):

            @pl.when(c * parts + part < leave)
            def _():
                start(y_copies(n, c * parts + part))

    for n in range(STEPS - 1):
        if n == 1:
            sent(y_copies(0, 0))
        arrived(x_copies(n))
        arrived(z_copies(n))

        def inner(i):
            for y in range(1, ny - 1):
                one_line(n, y, i)

        def outer(c):
            arrived(y_copies(n, c))

            def line(k):
                for y in (0, ny - 1):
                    one_line(n, y, c * LINES[n] + k)

            each(0, LINES[n], line)

        def outer_and_send(c):
            outer(c)
            send_piece(n + 1, c - 1)

        each(0, nx, inner)
        outer(0)
        each(1, pieces[n], outer_and_send)
        start(x_copies(n + 1))
        start(z_copies(n + 1))
        send_piece(n + 1, pieces[n] - 1)

    n = STEPS - 1
    each(0, pieces[n - 1], lambda c: sent(y_copies(n - 1, c)))
    sent(x_copies(n - 1))
    arrived(x_copies(n))
    arrived(z_copies(n))

    def all_inner_stats():
        return [
            remote(inner_stats.at[0], inner_stats.at[d], i_send.at[d - 1], i_recv.at[d - 1], ring("slabs", d))
            for d in range(1, lax.axis_size("slabs"))
        ]

    def inner_piece(c):
        for k in range(L):
            for p, y in enumerate(INNER):
                line_stats(inner_stats, one_line(n, y, c * L + k), c, 2 * k + p)

    def last(c):
        arrived(y_copies(n, c))
        for k in range(L):
            for p, y in enumerate((0, ny - 1)):
                line_stats(outer_stats, one_line(n, y, c * L + k), c, 2 * k + p)
        start(stat_copies(outer_stats, s_send, s_recv, c))

    each(0, pieces[n], inner_piece)
    start(all_inner_stats())
    each(0, begin, last)
    each(begin, leave, lambda c: arrived(y_copies(n, c)))
    each(0, leave, lambda c: sent(y_copies(n, c)))
    each(1, pieces[0], lambda c: sent(y_copies(0, c)))
    sent(x_copies(0))
    sent(x_copies(n))
    for m in range(STEPS):
        sent(z_copies(m))

    def drain(c):
        sent(stat_copies(outer_stats, s_send, s_recv, c))
        arrived(stat_copies(outer_stats, s_send, s_recv, c))

    each(0, begin, drain)
    sent(all_inner_stats())
    arrived(all_inner_stats())


def second_kernel(
    even, z_end, mobility, source, after, rest, stats,
    mob, src, halo, y_send, y_recv, s_send, s_recv, local,
):
    ny, nx, nz, _ = mobility.shape
    pieces = nx // L
    leave = leaving()
    begin = beginning()

    def loads(c):
        there, here = pl.ds(c * L, L), pl.ds((c - begin) * L, L)
        return [
            pltpu.make_async_copy(whole.at[y, there], part.at[p, here], local.at[q, p, c - begin])
            for q, (whole, part) in enumerate(((mobility, mob), (source, src)))
            for p, y in enumerate((0, ny - 1))
        ]

    def y_copies(c):
        lines, landing = pl.ds(1 + c * L, L), pl.ds((c - leave) * L, L)
        p = c - leave
        return (
            remote(even.at[ny, lines], halo.at[0, landing], y_send.at[0, p], y_recv.at[0, p], ring("rows", 1)),
            remote(even.at[1, lines], halo.at[1, landing], y_send.at[1, p], y_recv.at[1, p], ring("rows", -1)),
        )

    def my_stats(c):
        return stat_copies(stats, s_send, s_recv, c - begin)

    @pl.when(begin < pieces)
    def _():
        met = greet([ring("rows", 1), ring("rows", -1)] + others())
        each(begin, pieces, lambda c: start(loads(c)))
        met()
        each(leave, pieces, lambda c: start(y_copies(c)))

        def piece(c, landed):
            for k in range(L):
                i = c * L + k
                r = (c - begin) * L + k
                for p, y in enumerate((0, ny - 1)):
                    below = halo[0, (c - leave) * L + k] if landed and p == 0 else even[y, i + 1]
                    above = halo[1, (c - leave) * L + k] if landed and p == 1 else even[y + 2, i + 1]
                    value = next_value(
                        even[y + 1, i + 1], below, above, even[y + 1, i], even[y + 1, i + 2],
                        z_end[0, y, pl.ds(i, 1)], z_end[1, y, pl.ds(i, 1)], mob[p, r], src[p, r],
                    )
                    rest[p, r] = value
                    line_stats(stats, value, c - begin, 2 * k + p)
            start(my_stats(c))

        def held(c):
            wait(loads(c))
            piece(c, False)

        def moved(c):
            wait(loads(c))
            arrived(y_copies(c))
            piece(c, True)

        each(begin, leave, held)
        each(leave, pieces, moved)
        each(leave, pieces, lambda c: sent(y_copies(c)))

        def drain(c):
            sent(my_stats(c))
            arrived(my_stats(c))

        each(begin, pieces, drain)


def write_planes(first, end, planes, stats, value_of, block_of, at, anomaly, field_end, held, sems):
    _, _, nz, _ = field_end.shape
    slabs = stats.shape[0]

    def field_copies(c):
        lines = pl.ds(c * L, L)
        return [pltpu.make_async_copy(block_of(c, p), field_end.at[y, lines], sems.at[0, y, c]) for p, y in enumerate(planes)]

    def anomaly_copies(c):
        lines = pl.ds(c * L, L)
        return [pltpu.make_async_copy(held.at[y, lines], anomaly.at[y, lines], sems.at[1, y, c]) for y in planes]

    def piece(c):
        means = [stats[d, c - at, 0] for d in range(slabs)]
        mean = sum(means[1:], means[0]) * (1.0 / slabs)
        spread = stats[0, c - at, 1]
        for d in range(1, slabs):
            spread = spread + stats[d, c - at, 1]
        for other in means:
            spread = spread + (other - mean) * (other - mean) * float(nz)
        scale = lax.rsqrt(spread * (1.0 / (nz * slabs)) + EPS)
        for k in range(L):
            for p, y in enumerate(planes):
                r = 2 * k + p
                held[y, c * L + k] = (value_of(c, k, p) - mean[r:r + 1]) * scale[r:r + 1]
        start(anomaly_copies(c))

    def done(c):
        wait(field_copies(c))
        wait(anomaly_copies(c))

    return (
        lambda: each(first, end, lambda c: start(field_copies(c))),
        lambda: each(first, end, piece),
        lambda: each(first, end, done),
    )


def first_write(odd, inner_stats, outer_stats, anomaly, field_end, after, held, sems):
    ny, nx = field_end.shape[:2]

    def from_odd(first, end, planes, stats):
        return write_planes(
            first, end, planes, stats,
            lambda c, k, p: odd[planes[p] + 1, c * L + k + 1],
            lambda c, p: odd.at[planes[p] + 1, pl.ds(c * L + 1, L)],
            0, anomaly, field_end, held, sems,
        )

    parts = (from_odd(0, nx // L, INNER, inner_stats), from_odd(0, beginning(), (0, ny - 1), outer_stats))
    for phase in zip(*parts):
        for run in phase:
            run()
    after[...] = jnp.zeros_like(after)


def second_write(rest, stats, _a, _f, anomaly, field_end, held, sems):
    ny, nx = field_end.shape[:2]
    begin = beginning()
    for run in write_planes(
        begin, nx // L, (0, ny - 1), stats,
        lambda c, k, p: rest[p, (c - begin) * L + k],
        lambda c, p: rest.at[p, pl.ds((c - begin) * L, L)],
        begin, anomaly, field_end, held, sems,
    ):
        run()


def near(x):
    return pltpu.with_memory_space_constraint(x, pltpu.VMEM)


def far(x):
    return pltpu.with_memory_space_constraint(x, pltpu.HBM)


def per_device(field, mobility, source):
    ny, nx, nz, levels = field.shape
    f32 = jnp.float32
    pieces = nx // L
    most = nx // min(LINES)
    slabs = lax.axis_size("slabs")
    any_space = pl.BlockSpec(memory_space=pl.ANY)
    vmem = pl.BlockSpec(memory_space=pltpu.VMEM)
    padded = (ny + 2, nx + 2, nz, levels)
    faces = (2, ny, nx, levels)
    left = pieces - min(leave - hold for leave, hold in zip(LEAVE, HOLD))
    coming = pieces - min(LEAVE)
    odd, even, z_end, inner_stats, outer_stats = pl.pallas_call(
        first_kernel,
        out_shape=(
            pltpu.VMEM(padded, f32),
            pltpu.VMEM(padded, f32),
            pltpu.VMEM(faces, f32),
            pltpu.VMEM((slabs, pieces, 2, L * 2, levels), f32),
            pltpu.VMEM((slabs, pieces, 2, L * 2, levels), f32),
        ),
        in_specs=[any_space] * 3,
        out_specs=(vmem,) * 5,
        scratch_shapes=[
            pltpu.VMEM(field.shape, f32),
            pltpu.VMEM(field.shape, f32),
            pltpu.VMEM((STEPS - 1, *faces), f32),
            pltpu.VMEM((STEPS, *faces), f32),
            DMA((STEPS, 2, most)),
            DMA((STEPS, 2, most)),
            DMA((STEPS, 2)),
            DMA((STEPS, 2)),
            DMA((STEPS, 2)),
            DMA((STEPS, 2)),
            DMA((slabs - 1,)),
            DMA((slabs - 1,)),
            DMA((slabs - 1, pieces)),
            DMA((slabs - 1, pieces)),
            DMA((7,)),
        ],
        name="steps",
        compiler_params=pltpu.CompilerParams(
            collective_id=0, has_side_effects=True, vmem_limit_bytes=22 * 2**20
        ),
    )(field, mobility, source)
    shape = jax.ShapeDtypeStruct(field.shape, f32)
    writing = dict(
        scratch_shapes=[pltpu.VMEM(field.shape, f32), DMA((2, ny, pieces))],
        compiler_params=pltpu.CompilerParams(vmem_limit_bytes=12 * 2**20),
    )
    anomaly, field_end, after = pl.pallas_call(
        first_write,
        out_shape=(shape, shape, jax.ShapeDtypeStruct((8, levels), f32)),
        in_specs=[vmem, vmem, vmem],
        out_specs=(any_space, any_space, vmem),
        name="write",
        **writing,
    )(near(odd), near(inner_stats), near(outer_stats))
    rest, stats = pl.pallas_call(
        second_kernel,
        out_shape=(
            pltpu.VMEM((2, left * L, nz, levels), f32),
            pltpu.VMEM((slabs, left, 2, L * 2, levels), f32),
        ),
        in_specs=[vmem, vmem, any_space, any_space, any_space],
        out_specs=(vmem, vmem),
        scratch_shapes=[
            pltpu.VMEM((2, left * L, nz, levels), f32),
            pltpu.VMEM((2, left * L, nz, levels), f32),
            pltpu.VMEM((2, coming * L, nz, levels), f32),
            DMA((2, coming)),
            DMA((2, coming)),
            DMA((slabs - 1, left)),
            DMA((slabs - 1, left)),
            DMA((2, 2, left)),
        ],
        name="rest",
        compiler_params=pltpu.CompilerParams(
            collective_id=1, has_side_effects=True, vmem_limit_bytes=16 * 2**20
        ),
    )(near(even), near(z_end), far(mobility), far(source), after)
    return pl.pallas_call(
        second_write,
        out_shape=(shape, shape),
        in_specs=[vmem, vmem, any_space, any_space],
        out_specs=(any_space, any_space),
        input_output_aliases={2: 0, 3: 1},
        name="write_rest",
        **writing,
    )(near(rest), near(stats), anomaly, field_end)


def solution(mesh):
    spec = P("rows", "cols", "slabs", None)
    return jax.shard_map(
        per_device, mesh=mesh, in_specs=(spec,) * 3, out_specs=(spec, spec), check_vma=False
    )
```
